64 devices in a mesh: batch: 4 (over x, y), row: 16 (over z, core).
Axes of the slice: x: 2, y: 2, z: 8, core: 2. Of those that a mesh axis runs over, the one named last changes fastest.
The devices are a block of a 4x4x8 slice.
Arguments:
- trans_mat: bfloat16 [16384, 4096], P(('batch', 'row')), parts along dimension 0
- teleport: float32 [16384, 1024], P(('batch', 'row')), parts along dimension 0
- dangling: int32 [16384], P(('batch', 'row')), parts along dimension 0
- damping: float32 [12], replicated
- rank_init: float32 [16384, 1024], P(('batch', 'row')), parts along dimension 0
Outputs:
- output: float32 [16384, 1024], P(('batch', 'row')), parts along dimension 0
There are 4 independent parts. The reference program is written for one: setup_inputs(seed, part) draws one part's arguments, and reference() takes and returns one part's arrays. A program takes and returns all parts, laid end to end along the dimension named above; an argument that names none is the same for every part.
All inputs are finite; a program needn't handle non-finite values.
Results may differ from the reference program's by a relative error of at most 0.001.
Values are sent between devices in bfloat16 or wider.
A program may use at most 768 MiB of HBM per device.

```python
import jax
import jax.numpy as jnp
from jax import lax

NODES = 4096
SEEDS = 1024
SWEEPS = 12


def setup_inputs(seed: int = 0, part: int = 0) -> dict:
    base_key = jax.random.key(seed)
    part_key = jax.random.fold_in(base_key, part)
    key_list = jax.random.split(part_key, 8)
    dangling = (jax.random.randint(key_list[0], (NODES,), 0, 100) < 20).astype(jnp.int32)
    popular = jnp.exp(0.8 * jax.random.normal(key_list[1], (NODES,), jnp.float32))
    weights = popular[:, None] * jnp.maximum(jax.random.uniform(key_list[2], (NODES, NODES), jnp.float32) - 0.5, 0.0)
    keep_cols = 1.0 - dangling.astype(jnp.float32)
    col_sum = jnp.sum(weights, axis=0)
    trans_mat = (weights * (keep_cols / jnp.maximum(col_sum, 1e-6))[None, :]).astype(jnp.bfloat16)
    tele_raw = jnp.exp(1.2 * jax.random.normal(key_list[3], (NODES, SEEDS), jnp.float32))
    teleport = tele_raw / jnp.mean(tele_raw, axis=0, keepdims=True)
    col_scale = jax.random.uniform(key_list[4], (1, SEEDS), jnp.float32, 0.3, 3.0)
    rank_init = col_scale * jax.random.uniform(key_list[5], (NODES, SEEDS), jnp.float32, 0.2, 1.8)
    damping = jax.random.uniform(jax.random.key(seed + 1), (SWEEPS,), jnp.float32, 0.75, 0.95)
    return {"trans_mat": trans_mat, "teleport": teleport, "dangling": dangling, "damping": damping, "rank_init": rank_init}


def reference(trans_mat, teleport, dangling, damping, rank_init):
    dang_float = dangling.astype(jnp.float32)

    def one_sweep(rank_cur, factor):
        prod_rows = jnp.dot(trans_mat, rank_cur.astype(jnp.bfloat16), preferred_element_type=jnp.float32)
        dang_mass = jnp.dot(dang_float, rank_cur, preferred_element_type=jnp.float32)
        rank_next = factor * prod_rows + (1.0 - factor) * teleport + (factor / NODES) * dang_mass[None, :]
        return rank_next, None

    rank_final, unused = lax.scan(one_sweep, rank_init, damping)
    return rank_final
```

```python
import functools

import jax
import jax.numpy as jnp
from jax import lax
from jax.experimental import pallas as pl
from jax.experimental.pallas import tpu as pltpu
from jax.sharding import PartitionSpec as P

F32 = jnp.float32
BF16 = jnp.bfloat16


def sweeps_kernel(chips, num_nodes, sweeps,
                  damp_ref, dang_ref, mat_ref, tele_ref, init_ref, out_ref,
                  mat_t, mat_nat, tele_raw, tele_t, init_f32, init_send, init_recv,
                  rank_own, rank_sib, part, mass_send, mass_recv, dang, mass_own, mass_sib, out_stage,
                  ring_send, ring_recv, tele_send, tele_recv, init_ssem, init_rsem, dang_send, dang_recv,
                  mass_ssem, mass_rsem, rank_send, rank_recv, sum_send, sum_recv, out_send, out_recv, load_sem):
    rows = init_ref.shape[0]
    width = init_ref.shape[1] // chips
    half = chips * rows
    num_chunks = 4
    chunk = 2 * half // num_chunks
    me = lax.axis_index("row")
    z = me // 2
    core = lax.rem(me, 2)
    sibling = {"row": me + 1 - 2 * core}

    def chip(offset):
        return lax.rem(z + offset + chips, chips)

    def peer(chip_index):
        return {"row": 2 * chip_index + core}

    def lanes(block, size):
        return pl.ds(pl.multiple_of(block * size, size), size)

    def remote(src, dst, ssem, rsem, device):
        return pltpu.make_async_remote_copy(src_ref=src, dst_ref=dst, send_sem=ssem, recv_sem=rsem,
                                            device_id=device, device_id_type=pl.DeviceIdType.MESH)

    load_mat = pltpu.make_async_copy(mat_ref, mat_nat, load_sem.at[0])
    load_init = pltpu.make_async_copy(init_ref, init_f32, load_sem.at[1])
    load_dang = pltpu.make_async_copy(dang_ref, dang.at[z], load_sem.at[2])
    load_tele = pltpu.make_async_copy(tele_ref.at[:, lanes(z, width)], tele_raw.at[z], load_sem.at[3])
    load_init.start()
    load_dang.start()
    load_mat.start()
    load_tele.start()

    barrier = pltpu.get_barrier_semaphore()
    for offset in range(1, chips):
        pl.semaphore_signal(barrier, inc=1, device_id=peer(chip(offset)), device_id_type=pl.DeviceIdType.MESH)
    pl.semaphore_signal(barrier, inc=1, device_id=sibling, device_id_type=pl.DeviceIdType.MESH)
    pl.semaphore_wait(barrier, chips)

    far_first = sorted(range(1, chips), key=lambda offset: -min(offset, chips - offset))

    def tele_copy(offset):
        return remote(tele_ref.at[:, lanes(chip(offset), width)], tele_raw.at[z],
                      tele_send.at[offset], tele_recv.at[offset], peer(chip(offset)))

    def init_copy(offset):
        return remote(init_send.at[chip(offset)], init_recv.at[z],
                      init_ssem.at[offset], init_rsem.at[offset], peer(chip(offset)))

    def dang_copy(offset):
        return remote(dang.at[z], dang.at[z], dang_send.at[offset], dang_recv.at[offset], peer(chip(offset)))

    def mass_copy(offset):
        return remote(mass_send.at[chip(offset)], mass_recv.at[z],
                      mass_ssem.at[offset], mass_rsem.at[offset], peer(chip(offset)))

    def ring_copy(direction, step, piece):
        sign = 1 - 2 * direction
        slot = mat_t.at[chip(-sign * step), pl.ds(piece * chunk, chunk), :]
        return remote(slot, slot, ring_send.at[direction, step, piece], ring_recv.at[direction, step + 1, piece],
                      peer(chip(sign)))

    def ring_pieces(direction, step):
        if step < chips // 2 - 1:
            return range(num_chunks)
        return range(num_chunks // 2) if direction == 0 else range(num_chunks // 2, num_chunks)

    for offset in far_first:
        tele_copy(offset).start()

    load_dang.wait()
    load_init.wait()
    dang_cols = jnp.transpose(jnp.broadcast_to(dang[z][0:1, :], (width, rows)))
    for j in range(chips):
        tile = init_f32[:, j * width:(j + 1) * width]
        init_send[j] = tile.astype(BF16)
        mass_send[j] = jnp.broadcast_to(jnp.sum(tile * dang_cols, axis=0, keepdims=True), (8, width))
    for offset in far_first:
        init_copy(offset).start()
        mass_copy(offset).start()
        dang_copy(offset).start()

    load_mat.wait()
    for piece in range(num_chunks):
        for k in range(piece * chunk // rows, (piece + 1) * chunk // rows):
            block = 2 * (k % chips) + k // chips
            mat_t[z, k * rows:(k + 1) * rows, :] = jnp.transpose(mat_nat[:, block * rows:(block + 1) * rows])
        for direction in range(2):
            ring_copy(direction, 0, piece).start()

    init_recv[z] = init_send[z]
    mass_recv[z] = mass_send[z]
    for offset in far_first:
        init_copy(offset).wait_recv()
    for j in range(chips):
        rank_own[0, :, j * rows:(j + 1) * rows] = jnp.transpose(init_recv[j])

    def rank_copy(slot, block):
        where = lanes(block, rows)
        return remote(rank_own.at[slot, :, where], rank_sib.at[slot, :, where],
                      rank_send.at[slot], rank_recv.at[slot], sibling)

    def rank_all(slot):
        return remote(rank_own.at[slot], rank_sib.at[slot], rank_send.at[slot], rank_recv.at[slot], sibling)

    def sum_copy(slot):
        return remote(mass_own.at[slot], mass_sib.at[slot], sum_send.at[slot], sum_recv.at[slot], sibling)

    rank_all(0).start()
    for offset in far_first:
        mass_copy(offset).wait_recv()
    mass_row = jnp.sum(mass_recv[...], axis=0)[0:1, :]
    mass_cols = jnp.transpose(jnp.broadcast_to(mass_row, (width, width)))
    first_lane = lax.broadcasted_iota(jnp.int32, (width, width), 1) == 0
    mass_own[0] = jnp.where(first_lane, mass_cols, 0.0)
    sum_copy(0).start()

    for offset in far_first:
        dang_copy(offset).wait_recv()
        tele_copy(offset).wait_recv()
    load_tele.wait()
    for j in range(chips):
        tele_t[j] = jnp.transpose(tele_raw[j])

    def mass_term(slot, factor):
        total = jnp.sum(mass_own[slot] + mass_sib[slot], axis=1, keepdims=True)
        return (factor / num_nodes) * total

    def own_part(slot, block):
        return jnp.dot(rank_own[slot], mat_t[block, pl.ds(pl.multiple_of(core * half, half), half), :],
                       preferred_element_type=F32)

    def sib_part(slot, block):
        return jnp.dot(rank_sib[slot], mat_t[block, pl.ds(pl.multiple_of((1 - core) * half, half), half), :],
                       preferred_element_type=F32)

    def next_rank(prod, block, factor, mass):
        return factor * prod + (1.0 - factor) * tele_t[block] + mass

    def masked(rank, block):
        prod = rank * dang[block][0:1, :]
        total = prod[:, :width]
        for j in range(1, rows // width):
            total = total + prod[:, j * width:(j + 1) * width]
        return total

    rank_all(0).wait()
    sum_copy(0).wait()
    factor0 = damp_ref[0]
    mass0 = mass_term(0, factor0)
    mass_own[1] = jnp.zeros((width, width), F32)

    def first_sweep_block(block):
        prod = own_part(0, block) + sib_part(0, block)
        rank = next_rank(prod, block, factor0, mass0)
        rank_own[1, :, lanes(block, rows)] = rank.astype(BF16)
        mass_own[1] = mass_own[1] + masked(rank, block)
        rank_copy(1, block).start()

    first_sweep_block(z)
    for step in range(1, chips // 2 + 1):
        for piece in range(num_chunks):
            for direction in range(2):
                if piece in ring_pieces(direction, step - 1):
                    ring_copy(direction, step - 1, piece).wait_recv()
                if step < chips // 2 and piece in ring_pieces(direction, step):
                    ring_copy(direction, step, piece).start()
        first_sweep_block(chip(-step))
        if step < chips // 2:
            first_sweep_block(chip(step))
    sum_copy(1).start()

    def sweep(t, carry):
        now = lax.rem(t, 2)
        later = 1 - now
        factor = damp_ref[t]
        for block in range(chips):
            part[block] = own_part(now, block)
        rank_all(now).wait()
        sum_copy(now).wait()
        mass = mass_term(now, factor)
        total = jnp.zeros((width, width), F32)
        for block in range(chips):
            prod = part[block] + sib_part(now, block)
            rank = next_rank(prod, block, factor, mass)
            rank_own[later, :, block * rows:(block + 1) * rows] = rank.astype(BF16)
            total = total + masked(rank, block)
            rank_copy(later, block).start()
        mass_own[later] = total
        sum_copy(later).start()
        return carry

    lax.fori_loop(1, sweeps - 1, sweep, 0)

    last = sweeps - 1
    now = last % 2
    factor = damp_ref[last]
    for block in range(chips):
        part[block] = own_part(now, block)
    rank_all(now).wait()
    sum_copy(now).wait()
    mass = mass_term(now, factor)

    def out_copy(offset):
        return remote(out_stage.at[chip(offset)], out_ref.at[:, lanes(z, width)],
                      out_send.at[offset], out_recv.at[offset], peer(chip(offset)))

    keep = pltpu.make_async_copy(out_stage.at[z], out_ref.at[:, lanes(z, width)], load_sem.at[0])
    for offset in far_first + [0]:
        block = chip(offset)
        prod = part[block] + sib_part(now, block)
        out_stage[block] = jnp.transpose(next_rank(prod, block, factor, mass))
        if offset:
            out_copy(offset).start()
        else:
            keep.start()

    for offset in far_first:
        tele_copy(offset).wait_send()
        init_copy(offset).wait_send()
        mass_copy(offset).wait_send()
        dang_copy(offset).wait_send()
    for step in range(chips // 2):
        for direction in range(2):
            for piece in ring_pieces(direction, step):
                ring_copy(direction, step, piece).wait_send()
    keep.wait()
    for offset in far_first:
        out_copy(offset).wait()


def solution(mesh):
    chips = mesh.shape["row"] // 2
    spec_rows = P(("batch", "row"), None)
    spec_vec = P(("batch", "row"))

    def local_sweeps(mat_rows, tele_rows, dang_rows, damping, start_rows):
        rows, num_nodes = mat_rows.shape
        width = start_rows.shape[1] // chips
        sweeps = damping.shape[0]
        dang_tile = jnp.broadcast_to(dang_rows.astype(F32)[None, :], (8, rows))
        dma = pltpu.SemaphoreType.DMA
        hbm = pl.BlockSpec(memory_space=pl.ANY)
        return pl.pallas_call(
            functools.partial(sweeps_kernel, chips, num_nodes, sweeps),
            out_shape=jax.ShapeDtypeStruct(start_rows.shape, F32),
            in_specs=[pl.BlockSpec(memory_space=pltpu.SMEM), hbm, hbm, hbm, hbm],
            out_specs=hbm,
            scratch_shapes=[
                pltpu.VMEM((chips, num_nodes, rows), BF16),
                pltpu.VMEM((rows, num_nodes), BF16),
                pltpu.VMEM((chips, rows, width), F32),
                pltpu.VMEM((chips, width, rows), F32),
                pltpu.VMEM(start_rows.shape, F32),
                pltpu.VMEM((chips, rows, width), BF16),
                pltpu.VMEM((chips, rows, width), BF16),
                pltpu.VMEM((2, width, chips * rows), BF16),
                pltpu.VMEM((2, width, chips * rows), BF16),
                pltpu.VMEM((chips, width, rows), F32),
                pltpu.VMEM((chips, 8, width), F32),
                pltpu.VMEM((chips, 8, width), F32),
                pltpu.VMEM((chips, 8, rows), F32),
                pltpu.VMEM((2, width, width), F32),
                pltpu.VMEM((2, width, width), F32),
                pltpu.VMEM((chips, rows, width), F32),
                dma((2, chips // 2, 4)), dma((2, chips // 2 + 1, 4)),
                dma((chips,)), dma((chips,)),
                dma((chips,)), dma((chips,)),
                dma((chips,)), dma((chips,)),
                dma((chips,)), dma((chips,)),
                dma((2,)), dma((2,)),
                dma((2,)), dma((2,)),
                dma((chips,)), dma((chips,)),
                dma((4,)),
            ],
            compiler_params=pltpu.CompilerParams(collective_id=0, has_side_effects=True),
        )(damping, dang_tile, mat_rows, tele_rows, start_rows)

    return jax.shard_map(local_sweeps, mesh=mesh, in_specs=(spec_rows, spec_rows, spec_vec, P(None), spec_rows),
                         out_specs=spec_rows, check_vma=False)
```

```python
import functools

import jax
import jax.numpy as jnp
from jax import lax
from jax.experimental import pallas as pl
from jax.experimental.pallas import tpu as pltpu
from jax.sharding import PartitionSpec as P

F32 = jnp.float32
BF16 = jnp.bfloat16


def sweeps_kernel(chips, num_nodes, sweeps,
                  damp_ref, dang_ref, mat_ref, tele_ref, init_ref, out_ref,
                  mat_t, mat_nat, tele_raw, tele_t, init_f32, init_send, init_recv,
                  rank_own, rank_sib, part, mass_send, mass_recv, dang, mass_own, mass_sib, out_stage,
                  ring_send, ring_recv, tele_send, tele_recv, init_ssem, init_rsem, dang_send, dang_recv,
                  mass_ssem, mass_rsem, rank_send, rank_recv, sum_send, sum_recv, out_send, out_recv, load_sem):
    rows = init_ref.shape[0]
    width = init_ref.shape[1] // chips
    half = chips * rows
    num_chunks = 4
    chunk = 2 * half // num_chunks
    me = lax.axis_index("row")
    z = me // 2
    core = lax.rem(me, 2)
    sibling = {"row": me + 1 - 2 * core}

    def chip(offset):
        return lax.rem(z + offset + chips, chips)

    def peer(chip_index):
        return {"row": 2 * chip_index + core}

    def lanes(block, size):
        return pl.ds(pl.multiple_of(block * size, size), size)

    def remote(src, dst, ssem, rsem, device):
        return pltpu.make_async_remote_copy(src_ref=src, dst_ref=dst, send_sem=ssem, recv_sem=rsem,
                                            device_id=device, device_id_type=pl.DeviceIdType.MESH)

    load_mat = pltpu.make_async_copy(mat_ref, mat_nat, load_sem.at[0])
    load_init = pltpu.make_async_copy(init_ref, init_f32, load_sem.at[1])
    load_dang = pltpu.make_async_copy(dang_ref, dang.at[z], load_sem.at[2])
    load_tele = pltpu.make_async_copy(tele_ref.at[:, lanes(z, width)], tele_raw.at[z], load_sem.at[3])
    load_init.start()
    load_dang.start()
    load_mat.start()
    load_tele.start()

    barrier = pltpu.get_barrier_semaphore()
    for offset in range(1, chips):
        pl.semaphore_signal(barrier, inc=1, device_id=peer(chip(offset)), device_id_type=pl.DeviceIdType.MESH)
    pl.semaphore_signal(barrier, inc=1, device_id=sibling, device_id_type=pl.DeviceIdType.MESH)
    pl.semaphore_wait(barrier, chips)

    far_first = sorted(range(1, chips), key=lambda offset: -min(offset, chips - offset))

    def tele_copy(offset):
        return remote(tele_ref.at[:, lanes(chip(offset), width)], tele_raw.at[z],
                      tele_send.at[offset], tele_recv.at[offset], peer(chip(offset)))

    def init_copy(offset):
        return remote(init_send.at[chip(offset)], init_recv.at[z],
                      init_ssem.at[offset], init_rsem.at[offset], peer(chip(offset)))

    def dang_copy(offset):
        return remote(dang.at[z], dang.at[z], dang_send.at[offset], dang_recv.at[offset], peer(chip(offset)))

    def mass_copy(offset):
        return remote(mass_send.at[chip(offset)], mass_recv.at[z],
                      mass_ssem.at[offset], mass_rsem.at[offset], peer(chip(offset)))

    def ring_copy(direction, step, piece):
        sign = 1 - 2 * direction
        slot = mat_t.at[chip(-sign * step), pl.ds(piece * chunk, chunk), :]
        return remote(slot, slot, ring_send.at[direction, step, piece], ring_recv.at[direction, step + 1, piece],
                      peer(chip(sign)))

    def ring_pieces(direction, step):
        if step < chips // 2 - 1:
            return range(num_chunks)
        return range(num_chunks // 2) if direction == 0 else range(num_chunks // 2, num_chunks)

    for offset in far_first:
        tele_copy(offset).start()

    load_dang.wait()
    load_init.wait()
    dang_cols = jnp.transpose(jnp.broadcast_to(dang[z][0:1, :], (width, rows)))
    for j in range(chips):
        tile = init_f32[:, j * width:(j + 1) * width]
        init_send[j] = tile.astype(BF16)
        mass_send[j] = jnp.broadcast_to(jnp.sum(tile * dang_cols, axis=0, keepdims=True), (8, width))
    for offset in far_first:
        init_copy(offset).start()
        mass_copy(offset).start()
        dang_copy(offset).start()

    load_mat.wait()
    for piece in range(num_chunks):
        for k in range(piece * chunk // rows, (piece + 1) * chunk // rows):
            block = 2 * (k % chips) + k // chips
            mat_t[z, k * rows:(k + 1) * rows, :] = jnp.transpose(mat_nat[:, block * rows:(block + 1) * rows])
        for direction in range(2):
            ring_copy(direction, 0, piece).start()

    init_recv[z] = init_send[z]
    mass_recv[z] = mass_send[z]
    for offset in far_first:
        init_copy(offset).wait_recv()
    for j in range(chips):
        rank_own[0, j] = jnp.transpose(init_recv[j])

    def rank_copy(slot, block):
        return remote(rank_own.at[slot, block], rank_sib.at[slot, block],
                      rank_send.at[slot], rank_recv.at[slot], sibling)

    def rank_some(slot, block, count):
        where = pl.ds(block, count)
        return remote(rank_own.at[slot, where], rank_sib.at[slot, where],
                      rank_send.at[slot], rank_recv.at[slot], sibling)

    def rank_all(slot):
        return remote(rank_own.at[slot], rank_sib.at[slot], rank_send.at[slot], rank_recv.at[slot], sibling)

    def sum_copy(slot):
        return remote(mass_own.at[slot], mass_sib.at[slot], sum_send.at[slot], sum_recv.at[slot], sibling)

    rank_all(0).start()
    for offset in far_first:
        mass_copy(offset).wait_recv()
    mass_row = jnp.sum(mass_recv[...], axis=0)[0:1, :]
    mass_cols = jnp.transpose(jnp.broadcast_to(mass_row, (width, width)))
    first_lane = lax.broadcasted_iota(jnp.int32, (width, width), 1) == 0
    mass_own[0] = jnp.where(first_lane, mass_cols, 0.0)
    sum_copy(0).start()

    for offset in far_first:
        dang_copy(offset).wait_recv()
        tele_copy(offset).wait_recv()
    load_tele.wait()
    for j in range(chips):
        tele_t[j] = jnp.transpose(tele_raw[j])

    def mass_term(slot, factor):
        total = jnp.sum(mass_own[slot] + mass_sib[slot], axis=1, keepdims=True)
        return (factor / num_nodes) * total

    def joined(rank, slot):
        return jnp.concatenate([rank[slot, k] for k in range(chips)], axis=1)

    def own_part(slot, block):
        return jnp.dot(joined(rank_own, slot), mat_t[block, pl.ds(pl.multiple_of(core * half, half), half), :],
                       preferred_element_type=F32)

    def sib_part(slot, block):
        return jnp.dot(joined(rank_sib, slot), mat_t[block, pl.ds(pl.multiple_of((1 - core) * half, half), half), :],
                       preferred_element_type=F32)

    def next_rank(prod, block, factor, mass):
        return factor * prod + (1.0 - factor) * tele_t[block] + mass

    def masked(rank, block):
        prod = rank * dang[block][0:1, :]
        total = prod[:, :width]
        for j in range(1, rows // width):
            total = total + prod[:, j * width:(j + 1) * width]
        return total

    rank_all(0).wait()
    sum_copy(0).wait()
    factor0 = damp_ref[0]
    mass0 = mass_term(0, factor0)
    mass_own[1] = jnp.zeros((width, width), F32)

    def first_sweep_block(block):
        prod = own_part(0, block) + sib_part(0, block)
        rank = next_rank(prod, block, factor0, mass0)
        rank_own[1, block] = rank.astype(BF16)
        mass_own[1] = mass_own[1] + masked(rank, block)
        rank_copy(1, block).start()

    first_sweep_block(z)
    for step in range(1, chips // 2 + 1):
        for piece in range(num_chunks):
            for direction in range(2):
                if piece in ring_pieces(direction, step - 1):
                    ring_copy(direction, step - 1, piece).wait_recv()
                if step < chips // 2 and piece in ring_pieces(direction, step):
                    ring_copy(direction, step, piece).start()
        first_sweep_block(chip(-step))
        if step < chips // 2:
            first_sweep_block(chip(step))
    sum_copy(1).start()

    def sweep(t, carry):
        now = lax.rem(t, 2)
        later = 1 - now
        factor = damp_ref[t]
        for block in range(chips):
            part[block] = own_part(now, block)
        rank_all(now).wait()
        sum_copy(now).wait()
        mass = mass_term(now, factor)
        total = jnp.zeros((width, width), F32)
        prod = None
        for ahead in range(chips + 1):
            done = prod
            if ahead < chips:
                prod = part[ahead] + sib_part(now, ahead)
            if ahead:
                block = ahead - 1
                rank = next_rank(done, block, factor, mass)
                rank_own[later, block] = rank.astype(BF16)
                total = total + masked(rank, block)
                if block == 5:
                    rank_some(later, 0, 6).start()
                if block == 7:
                    rank_some(later, 6, 2).start()
        mass_own[later] = total
        sum_copy(later).start()
        return carry

    lax.fori_loop(1, sweeps - 1, sweep, 0)

    last = sweeps - 1
    now = last % 2
    factor = damp_ref[last]
    for block in range(chips):
        part[block] = own_part(now, block)
    rank_all(now).wait()
    sum_copy(now).wait()
    mass = mass_term(now, factor)

    def out_copy(offset):
        return remote(out_stage.at[chip(offset)], out_ref.at[:, lanes(z, width)],
                      out_send.at[offset], out_recv.at[offset], peer(chip(offset)))

    keep = pltpu.make_async_copy(out_stage.at[z], out_ref.at[:, lanes(z, width)], load_sem.at[0])
    for offset in far_first + [0]:
        block = chip(offset)
        prod = part[block] + sib_part(now, block)
        out_stage[block] = jnp.transpose(next_rank(prod, block, factor, mass))
        if offset:
            out_copy(offset).start()
        else:
            keep.start()

    for offset in far_first:
        tele_copy(offset).wait_send()
        init_copy(offset).wait_send()
        mass_copy(offset).wait_send()
        dang_copy(offset).wait_send()
    for step in range(chips // 2):
        for direction in range(2):
            for piece in ring_pieces(direction, step):
                ring_copy(direction, step, piece).wait_send()
    keep.wait()
    for offset in far_first:
        out_copy(offset).wait()


def solution(mesh):
    chips = mesh.shape["row"] // 2
    spec_rows = P(("batch", "row"), None)
    spec_vec = P(("batch", "row"))

    def local_sweeps(mat_rows, tele_rows, dang_rows, damping, start_rows):
        rows, num_nodes = mat_rows.shape
        width = start_rows.shape[1] // chips
        sweeps = damping.shape[0]
        dang_tile = jnp.broadcast_to(dang_rows.astype(F32)[None, :], (8, rows))
        dma = pltpu.SemaphoreType.DMA
        hbm = pl.BlockSpec(memory_space=pl.ANY)
        return pl.pallas_call(
            functools.partial(sweeps_kernel, chips, num_nodes, sweeps),
            out_shape=jax.ShapeDtypeStruct(start_rows.shape, F32),
            in_specs=[pl.BlockSpec(memory_space=pltpu.SMEM), hbm, hbm, hbm, hbm],
            out_specs=hbm,
            scratch_shapes=[
                pltpu.VMEM((chips, num_nodes, rows), BF16),
                pltpu.VMEM((rows, num_nodes), BF16),
                pltpu.VMEM((chips, rows, width), F32),
                pltpu.VMEM((chips, width, rows), F32),
                pltpu.VMEM(start_rows.shape, F32),
                pltpu.VMEM((chips, rows, width), BF16),
                pltpu.VMEM((chips, rows, width), BF16),
                pltpu.VMEM((2, chips, width, rows), BF16),
                pltpu.VMEM((2, chips, width, rows), BF16),
                pltpu.VMEM((chips, width, rows), F32),
                pltpu.VMEM((chips, 8, width), F32),
                pltpu.VMEM((chips, 8, width), F32),
                pltpu.VMEM((chips, 8, rows), F32),
                pltpu.VMEM((2, width, width), F32),
                pltpu.VMEM((2, width, width), F32),
                pltpu.VMEM((chips, rows, width), F32),
                dma((2, chips // 2, 4)), dma((2, chips // 2 + 1, 4)),
                dma((chips,)), dma((chips,)),
                dma((chips,)), dma((chips,)),
                dma((chips,)), dma((chips,)),
                dma((chips,)), dma((chips,)),
                dma((2,)), dma((2,)),
                dma((2,)), dma((2,)),
                dma((chips,)), dma((chips,)),
                dma((4,)),
            ],
            compiler_params=pltpu.CompilerParams(collective_id=0, has_side_effects=True),
        )(damping, dang_tile, mat_rows, tele_rows, start_rows)

    return jax.shard_map(local_sweeps, mesh=mesh, in_specs=(spec_rows, spec_rows, spec_vec, P(None), spec_rows),
                         out_specs=spec_rows, check_vma=False)
```
